32 devices in a mesh: groups: 2 (over y), ep: 16 (over z, x, core).
Axes of the slice: x: 2, y: 2, z: 4, core: 2. Of those that a mesh axis runs over, the one named last changes fastest.
Arguments:
- tokens: bfloat16 [512, 2880], P(('groups', 'ep')), parts along dimension 0, may hold values from -6 to 6
- routes: int32 [512, 4], P(('groups', 'ep')), parts along dimension 0, may hold values from 0 to 7, all different within a row; in each aligned block of 16 rows (0 to 15, 16 to 31, ...) at most 16 rows name the same one
- gate_fixed: int32 [512, 4], P(('groups', 'ep')), parts along dimension 0, may hold values from 1 to 65535
- gate_weight: bfloat16 [16, 2880, 720], P('ep'), may hold values from -0.109375 to 0.109375
- up_weight: bfloat16 [16, 2880, 720], P('ep'), may hold values from -0.109375 to 0.109375
- down_weight: bfloat16 [16, 720, 2880], P('ep'), may hold values from -0.15625 to 0.15625
Outputs:
- mixed: bfloat16 [512, 2880], P(('groups', 'ep')), parts along dimension 0
The draws below stay inside these ranges and needn't reach their ends.
There are 2 independent parts, one for each index of `groups`. The reference program is written for one: setup_inputs(seed, part) draws one part's arguments, and reference() takes and returns one part's arrays. A program takes and returns all parts, laid end to end along the dimension named above; an argument that names none is the same for every part. Nothing has to cross between parts.
Inputs may be any that keep to these rules, and one draw needn't show every extreme that they name: `routes`: each row names 4 different experts; the 16 rows of one device name any one expert at most 16 times.
All inputs are finite; a program needn't handle non-finite values.
Results may differ from the reference program's by a relative error of at most 0.0065.
Values may be sent and summed in bfloat16 or wider, within the bound.
No kernel may reach another device: no remote copies, remote signals or barrier semaphores. Data moves between devices by JAX's collectives and lax.ppermute only.
A program may use at most 64 MiB of HBM per device.

```python
import math
import jax
import jax.numpy as jnp
import numpy as np
from jax import lax

D = 2880
FF = 1440
TOP = 4
TOK_DEV = 16
HALF = 720
EXPERTS = 8
TOKENS = 256
CAP = 16
N_EP = 16


def set_ends(values, stream_key, least, high):
    longest = values.shape.index(max(values.shape))
    spots = []
    for shift in (0, 1):
        where = [jax.random.randint(jax.random.fold_in(stream_key, axis), (), 0, length) for axis, length in enumerate(values.shape)]
        where[longest] = (where[longest] + shift) % values.shape[longest]
        spots.append(tuple(where))
    return values.at[spots[0]].set(least).at[spots[1]].set(high)


def block_levels(rng, extent, split, least, top_value):
    level, own = 1.0, jax.random.fold_in(rng, 6)
    for dim, parts in split:
        steps = jnp.exp(jax.random.uniform(jax.random.fold_in(own, dim), (parts,), jnp.float32, least / len(split), top_value / len(split)))
        level = level * jnp.repeat(steps, extent[dim] // parts).reshape([-1 if axis == dim else 1 for axis in range(len(extent))])
    return level


def shared_out(stream_key, own, number, rows, amount, top, reach, lean):
    sequence = jax.random.permutation(stream_key, amount)
    heavy_load, ordinary = shares(amount, rows * top, reach, lean, True), shares(amount, rows * top, reach, lean, False)
    places = jnp.arange(amount)

    def named(lengths, turn):
        used = int((lengths > 0).sum())
        fixed = max(1, used // 4)
        moved = fixed + (places - fixed + turn * (used - fixed)) % max(1, amount - fixed)
        return jnp.zeros((amount,), jnp.int32).at[sequence[jnp.where(places < fixed, places, moved)]].set(jnp.asarray(lengths, jnp.int32))

    lengths = jnp.where(number % 4 == 0, named(heavy_load, number // 4), named(ordinary, number - number // 4 - 1))
    mixed = jax.random.permutation(jax.random.fold_in(own, 3), amount)
    giver, receiver = mixed[0:amount // 2 * 2:2], mixed[1:amount // 2 * 2:2]
    margin = jnp.minimum(lengths[giver] - 1, reach - lengths[receiver]) // 2
    margin = jnp.where((giver == sequence[0]) | (receiver == sequence[0]) | (lengths[receiver] == 0), 0, jnp.maximum(margin, 0))
    moved = jax.random.randint(jax.random.fold_in(own, 4), (amount // 2,), 0, 1 << 20) % (margin + 1)
    lengths = lengths.at[giver].add(-moved).at[receiver].add(moved)
    members = jnp.searchsorted(jnp.cumsum(lengths), jnp.arange(rows * top), side="right").astype(jnp.int32)
    grid = members.reshape(top, rows).T
    grid = grid[jax.random.permutation(jax.random.fold_in(own, 1), rows)]
    turn = jax.random.randint(jax.random.fold_in(own, 2), (rows, 1), 0, top)
    return jnp.take_along_axis(grid, (jnp.arange(top)[None, :] + turn) % top, axis=1)


def shares(count, total, limit, lean, full):
    weights = [(1 << 20) // math.isqrt(standing ** lean) + 1 for standing in range(1, count + 1)]
    largest = limit if full else min(limit, max(-(-total // count), total * weights[0] // sum(weights)))
    least = 1 if total - largest >= count - 1 else 0
    given, surplus = [largest] + [least] * (count - 1), total - largest - least * (count - 1)
    while surplus > 0:
        free = [i for i in range(1, count) if given[i] < largest] or [i for i in range(1, count) if given[i] < limit]
        pool, budget = sum([weights[i] for i in free]), surplus
        for i in free:
            more = min(limit - given[i], max(1, budget * weights[i] // pool), surplus)
            given[i] = given[i] + more
            surplus = surplus - more
    return np.array(given)


def noise(own_key, dims, spread, limit, shards=(), kind=jnp.bfloat16):
    drawn = jax.random.normal(own_key, dims, jnp.float32) * spread
    if len(shards) > 0:
        drawn = block_levels(own_key, dims, shards, -0.22, 0.18) * drawn
    return jnp.clip(drawn, min=-limit, max=limit).astype(kind)


def setup_inputs(seed: int = 0, part: int = 0) -> dict:
    streams_of = jax.random.split(jax.random.key(seed), 7)
    part_keys = jax.random.split(jax.random.fold_in(streams_of[6], part), 7)
    tokens = noise(part_keys[0], (TOKENS, D), 1.0, 6.0, ((0, 16),))
    routes_keys = jax.random.split(jax.random.fold_in(part_keys[1], 1), TOKENS // TOK_DEV)
    routes_turns = jax.random.permutation(jax.random.fold_in(part_keys[1], 3), TOKENS // TOK_DEV)
    routes = jax.vmap(lambda own, number: shared_out(jax.random.fold_in(part_keys[1], 2), own, number, TOK_DEV, EXPERTS, TOP, CAP, 2))(routes_keys, routes_turns).reshape((TOKENS, TOP))
    gate_fixed = set_ends(jax.random.randint(part_keys[2], (TOKENS, TOP), 1, 65536), jax.random.fold_in(part_keys[2], 1), 1, 65535).astype(jnp.int32)
    gate_weight = noise(streams_of[3], (N_EP, D, HALF), D ** -0.5, 0.109375, ((0, 16),))
    up_weight = noise(streams_of[4], (N_EP, D, HALF), D ** -0.5, 0.109375, ((0, 16),))
    down_weight = noise(streams_of[5], (N_EP, HALF, D), FF ** -0.5, 0.15625, ((0, 16),))
    return dict(tokens=tokens, routes=routes, gate_fixed=gate_fixed, gate_weight=gate_weight, up_weight=up_weight, down_weight=down_weight)


def reference(tokens, routes, gate_fixed, gate_weight, up_weight, down_weight):
    experts = N_EP // 2
    onehot = (routes[:, :, None] == jnp.arange(experts, dtype=jnp.int32)).astype(jnp.int32)
    grouped = onehot.reshape(N_EP, TOK_DEV * TOP, experts)
    before = jnp.cumsum(grouped, axis=1) - grouped
    position = jnp.sum(before * grouped, axis=-1).reshape(TOKENS, TOP).astype(jnp.int32)
    source = (jnp.arange(TOKENS, dtype=jnp.int32) // TOK_DEV)[:, None]
    column = (source * CAP + position).astype(jnp.int32)
    token_ids = jnp.broadcast_to(jnp.arange(TOKENS, dtype=jnp.int32)[:, None], (TOKENS, TOP))
    slot_table = jnp.full((experts, N_EP * CAP), TOKENS, jnp.int32).at[routes, column].set(token_ids)
    padded = jnp.concatenate([tokens, jnp.zeros((1, D), tokens.dtype)], axis=0)

    def half_part(expert_rows, index):
        w_gate = lax.dynamic_index_in_dim(gate_weight, index, 0, keepdims=False)
        w_up = lax.dynamic_index_in_dim(up_weight, index, 0, keepdims=False)
        w_down = lax.dynamic_index_in_dim(down_weight, index, 0, keepdims=False)
        gate_part = jnp.dot(expert_rows, w_gate, preferred_element_type=jnp.float32)
        up_part = jnp.dot(expert_rows, w_up, preferred_element_type=jnp.float32)
        hidden = (jax.nn.silu(gate_part) * up_part).astype(jnp.bfloat16)
        return jnp.dot(hidden, w_down, preferred_element_type=jnp.float32).astype(jnp.bfloat16)

    def run_expert(expert):
        expert_rows = padded[slot_table[expert]]
        first = (2 * expert).astype(jnp.int32)
        lower = half_part(expert_rows, first)
        upper = half_part(expert_rows, (first + 1).astype(jnp.int32))
        return (lower.astype(jnp.float32) + upper.astype(jnp.float32)).astype(jnp.bfloat16)

    outputs = lax.map(run_expert, jnp.arange(experts, dtype=jnp.int32))
    picked = outputs[routes, column]
    weights = gate_fixed.astype(jnp.float32) / 65536.0
    mixed = jnp.sum(weights[:, :, None] * picked.astype(jnp.float32), axis=1)
    return mixed.astype(jnp.bfloat16)
```

```python
import jax
import jax.numpy as jnp
from jax import lax
from jax.experimental import pallas as pl
from jax.experimental.pallas import tpu as pltpu
from jax.sharding import PartitionSpec as P


def swapped(value, axis, bit):
    mask = 2**bit
    pairs = [(source, source ^ mask) for source in range(lax.axis_size(axis))]
    return lax.ppermute(value, axis, pairs)


def turned(value, axis, step):
    size = lax.axis_size(axis)
    pairs = [(source, (source + 4 * step) % size) for source in range(size)]
    return lax.ppermute(value, axis, pairs)


def expert_half(expert_rows, w_gate, w_up, w_down):
    gate_part = jnp.dot(expert_rows, w_gate, preferred_element_type=jnp.float32)
    up_part = jnp.dot(expert_rows, w_up, preferred_element_type=jnp.float32)
    hidden = (jax.nn.silu(gate_part) * up_part).astype(jnp.bfloat16)
    return jnp.dot(hidden, w_down, preferred_element_type=jnp.float32).astype(jnp.bfloat16)


def slotted(tokens, routes, gate_fixed, gate_weight, up_weight, down_weight, capacity):
    devices_ep = lax.axis_size("ep")
    experts = devices_ep // 2
    tok_count = tokens.shape[0]
    top_count = routes.shape[1]
    width = tokens.shape[1]
    onehot = (routes[:, :, None] == jnp.arange(experts, dtype=jnp.int32)).astype(jnp.int32)
    flat_hot = onehot.reshape(tok_count * top_count, experts)
    before = jnp.cumsum(flat_hot, axis=0) - flat_hot
    position = jnp.sum(before * flat_hot, axis=1).reshape(tok_count, top_count)
    slot_index = routes * capacity + position
    select = (slot_index[:, :, None] == jnp.arange(experts * capacity, dtype=jnp.int32)).astype(
        jnp.int32
    )
    select = jnp.sum(select, axis=1).astype(jnp.bfloat16)
    packed = jnp.einsum("ts,td->sd", select, tokens, preferred_element_type=jnp.float32).astype(
        jnp.bfloat16
    )
    packed = packed.reshape(experts, 1, capacity, width)
    outgoing = jnp.broadcast_to(packed, (experts, 2, capacity, width)).reshape(
        devices_ep, capacity, width
    )
    received = lax.all_to_all(outgoing, "ep", split_axis=0, concat_axis=0, tiled=True)
    result = expert_half(received.reshape(-1, width), gate_weight[0], up_weight[0], down_weight[0])
    partial_value = result.reshape(received.shape[0], received.shape[1], width)
    parity = lax.axis_index("ep") % 2
    halves = partial_value.reshape(devices_ep, capacity, 2, width // 2)
    kept_half = lax.dynamic_index_in_dim(halves, parity, 2, keepdims=False)
    given_half = lax.dynamic_index_in_dim(halves, 1 - parity, 2, keepdims=False)
    partner = swapped(given_half, "ep", 0)
    reduced = (kept_half.astype(jnp.float32) + partner.astype(jnp.float32)).astype(jnp.bfloat16)
    returned = lax.all_to_all(reduced, "ep", split_axis=0, concat_axis=0, tiled=True)
    ordered = returned.reshape(experts, 2, capacity, width // 2).transpose(0, 2, 1, 3)
    expert_out = ordered.reshape(experts * capacity, width)
    picked = jnp.take(expert_out, slot_index.reshape(-1), axis=0).reshape(
        tok_count, top_count, width
    )
    weights = gate_fixed.astype(jnp.float32) / 65536.0
    mixed = jnp.sum(weights[:, :, None] * picked.astype(jnp.float32), axis=1)
    return mixed.astype(jnp.bfloat16)


def pieces_of(extent, limit, unit):
    count = -(-extent // limit)
    step = -(-extent // (count * unit)) * unit
    return [(start, min(step, extent - start)) for start in range(0, extent, step)]


def pack_tokens(tokens, routes, gate_fixed, experts):
    count, width = tokens.shape
    top = routes.shape[1]

    def kernel(tok_ref, route_ref, gate_ref, out_ref):
        rows = lax.broadcasted_iota(jnp.int32, (experts, count), 0)
        share = jnp.zeros((experts, count), jnp.float32)
        for k in range(top):
            value = gate_ref[k : k + 1, :].astype(jnp.float32) * (1.0 / 65536.0)
            share = share + jnp.where(route_ref[k : k + 1, :] == rows, value, 0.0)
        high = share.astype(jnp.bfloat16)
        low = (share - high.astype(jnp.float32)).astype(jnp.bfloat16)
        both = jnp.concatenate([high.astype(jnp.float32), low.astype(jnp.float32)], axis=0)
        unit = (
            lax.broadcasted_iota(jnp.int32, (count, count), 0)
            == lax.broadcasted_iota(jnp.int32, (count, count), 1)
        ).astype(jnp.bfloat16)
        columns = lax.dot_general(
            unit,
            both.astype(jnp.bfloat16),
            (((1,), (1,)), ((), ())),
            preferred_element_type=jnp.float32,
        )
        out_ref[:, :width] = tok_ref[...]
        out_ref[:, width:] = columns.astype(jnp.bfloat16)

    return pl.pallas_call(
        kernel,
        out_shape=jax.ShapeDtypeStruct((count, width + 2 * experts), jnp.bfloat16),
        in_specs=[pl.BlockSpec(memory_space=pltpu.VMEM)] * 3,
        out_specs=pl.BlockSpec(memory_space=pltpu.VMEM),
        name="pack_tokens",
    )(tokens, routes.T, gate_fixed.T)


def expert_chunks(chunks, expert, w_gate, w_up, w_down, width):
    count = chunks[0].shape[0]
    wide = chunks[0].shape[1]
    experts = (wide - width) // 2
    number = len(chunks)
    rows = number * count
    units = w_gate.shape[0]
    h_tiles = pieces_of(units, 256, 16)
    d_tiles = pieces_of(width, 768, 128)
    tail = width // 128 * 128

    def kernel(*refs):
        expert_ref = refs[0]
        in_refs = refs[1 : 1 + number]
        wg_ref, wu_ref, wd_ref = refs[1 + number : 4 + number]
        out_refs = refs[4 + number : 4 + 2 * number]
        x_ref, g_ref, u_ref, d_ref, t_ref, sem = refs[4 + 2 * number :]
        loads = []
        for n, (start, size) in enumerate(h_tiles):
            for m, (source, place) in enumerate(((wg_ref, g_ref), (wu_ref, u_ref))):
                copy = pltpu.make_async_copy(
                    source.at[pl.ds(start, size)], place.at[pl.ds(start, size)], sem.at[2 * n + m]
                )
                copy.start()
                loads.append(copy)
        downs = []
        for n, (start, size) in enumerate(d_tiles):
            copy = pltpu.make_async_copy(
                wd_ref.at[:, pl.ds(start, size)],
                d_ref.at[:, pl.ds(start, size)],
                sem.at[2 * len(h_tiles) + n],
            )
            copy.start()
            downs.append(copy)
        for n in range(number):
            x_ref[n * count : (n + 1) * count, :] = in_refs[n][...]
        lanes = lax.broadcasted_iota(jnp.int32, (8, wide - tail), 1) - (width - tail)
        mine = (lanes == expert_ref[0]) | (lanes == expert_ref[0] + experts)
        share = lax.dot_general(
            jnp.where(mine, 1.0, 0.0).astype(jnp.bfloat16),
            x_ref[:, tail:],
            (((1,), (1,)), ((), ())),
            preferred_element_type=jnp.float32,
        )[0:1, :]
        x = x_ref[:, :width]
        nt = (((1,), (1,)), ((), ()))
        for n, (start, size) in enumerate(h_tiles):
            loads[2 * n].wait()
            gate = lax.dot_general(
                g_ref[start : start + size, :], x, nt, preferred_element_type=jnp.float32
            )
            loads[2 * n + 1].wait()
            up = lax.dot_general(
                u_ref[start : start + size, :], x, nt, preferred_element_type=jnp.float32
            )
            hidden = gate / (1.0 + jnp.exp(-gate)) * up * share
            t_ref[start : start + size, :] = hidden
        hidden = t_ref[...].T.astype(jnp.bfloat16)
        for n, (start, size) in enumerate(d_tiles):
            downs[n].wait()
            part = jnp.dot(
                hidden, d_ref[:, start : start + size], preferred_element_type=jnp.float32
            ).astype(jnp.bfloat16)
            for m in range(number):
                out_refs[m][:, start : start + size] = part[m * count : (m + 1) * count, :]

    vmem = pl.BlockSpec(memory_space=pltpu.VMEM)
    return pl.pallas_call(
        kernel,
        out_shape=[jax.ShapeDtypeStruct((count, width), jnp.bfloat16)] * number,
        in_specs=[pl.BlockSpec(memory_space=pltpu.SMEM)]
        + [vmem] * number
        + [pl.BlockSpec(memory_space=pl.ANY)] * 3,
        out_specs=[vmem] * number,
        scratch_shapes=[
            pltpu.VMEM((rows, wide), jnp.bfloat16),
            pltpu.VMEM((units, width), jnp.bfloat16),
            pltpu.VMEM((units, width), jnp.bfloat16),
            pltpu.VMEM((units, width), jnp.bfloat16),
            pltpu.VMEM((units, rows), jnp.float32),
            pltpu.SemaphoreType.DMA((2 * len(h_tiles) + len(d_tiles),)),
        ],
        compiler_params=pltpu.CompilerParams(vmem_limit_bytes=40 * 2**20),
        name="expert_chunks",
    )(expert, *chunks, w_gate, w_up, w_down)


def added(*values):
    total = values[0].astype(jnp.float32)
    for value in values[1:]:
        total = total + value.astype(jnp.float32)
    return total.astype(jnp.bfloat16)


def dense(tokens, routes, gate_fixed, gate_weight, up_weight, down_weight):
    devices_ep = lax.axis_size("ep")
    layers = devices_ep // 4
    width = tokens.shape[1]
    own = pack_tokens(tokens, routes, gate_fixed, devices_ep // 2)
    near = [own] + [turned(own, "ep", k) for k in range(1, layers)]
    far = [swapped(value, "ep", 1) for value in near]
    mine = near + far
    theirs = [swapped(value, "ep", 0) for value in mine]
    expert = (lax.axis_index("ep") // 2).astype(jnp.int32).reshape(1)
    parts = expert_chunks(
        mine + theirs,
        expert,
        gate_weight[0].T,
        up_weight[0].T,
        down_weight[0],
        width,
    )
    kept, given = parts[: len(mine)], parts[len(mine) :]
    back = [swapped(value, "ep", 0) for value in given]
    far_sums = [added(kept[layers + k], back[layers + k]) for k in range(layers)]
    from_far = [swapped(value, "ep", 1) for value in far_sums]
    near_sums = [added(kept[k], back[k], from_far[k]) for k in range(layers)]
    home = [turned(near_sums[k], "ep", -k) for k in range(1, layers)]
    return added(kept[0], back[0], from_far[0], *home)


def local(tokens, routes, gate_fixed, gate_weight, up_weight, down_weight):
    devices_ep = lax.axis_size("ep")
    tok_count, top_count = routes.shape
    capacity = min(tok_count, 2 * tok_count * top_count // (devices_ep // 2))
    if capacity == tok_count and devices_ep % 4 == 0:
        return dense(tokens, routes, gate_fixed, gate_weight, up_weight, down_weight)
    return slotted(tokens, routes, gate_fixed, gate_weight, up_weight, down_weight, capacity)


def solution(mesh):
    placed = (
        P(("groups", "ep"), None),
        P(("groups", "ep"), None),
        P(("groups", "ep"), None),
        P("ep", None, None),
        P("ep", None, None),
        P("ep", None, None),
    )
    return jax.shard_map(
        local, mesh=mesh, in_specs=placed, out_specs=P(("groups", "ep"), None), check_vma=False
    )
```

```python
import jax
import jax.numpy as jnp
from jax import lax
from jax.experimental import pallas as pl
from jax.experimental.pallas import tpu as pltpu
from jax.sharding import PartitionSpec as P


def swapped(value, axis, bit):
    mask = 2**bit
    pairs = [(source, source ^ mask) for source in range(lax.axis_size(axis))]
    return lax.ppermute(value, axis, pairs)


def turned(value, axis, step):
    size = lax.axis_size(axis)
    pairs = [(source, (source + 4 * step) % size) for source in range(size)]
    return lax.ppermute(value, axis, pairs)


def expert_half(expert_rows, w_gate, w_up, w_down):
    gate_part = jnp.dot(expert_rows, w_gate, preferred_element_type=jnp.float32)
    up_part = jnp.dot(expert_rows, w_up, preferred_element_type=jnp.float32)
    hidden = (jax.nn.silu(gate_part) * up_part).astype(jnp.bfloat16)
    return jnp.dot(hidden, w_down, preferred_element_type=jnp.float32).astype(jnp.bfloat16)


def slotted(tokens, routes, gate_fixed, gate_weight, up_weight, down_weight, capacity):
    devices_ep = lax.axis_size("ep")
    experts = devices_ep // 2
    tok_count = tokens.shape[0]
    top_count = routes.shape[1]
    width = tokens.shape[1]
    onehot = (routes[:, :, None] == jnp.arange(experts, dtype=jnp.int32)).astype(jnp.int32)
    flat_hot = onehot.reshape(tok_count * top_count, experts)
    before = jnp.cumsum(flat_hot, axis=0) - flat_hot
    position = jnp.sum(before * flat_hot, axis=1).reshape(tok_count, top_count)
    slot_index = routes * capacity + position
    select = (slot_index[:, :, None] == jnp.arange(experts * capacity, dtype=jnp.int32)).astype(
        jnp.int32
    )
    select = jnp.sum(select, axis=1).astype(jnp.bfloat16)
    packed = jnp.einsum("ts,td->sd", select, tokens, preferred_element_type=jnp.float32).astype(
        jnp.bfloat16
    )
    packed = packed.reshape(experts, 1, capacity, width)
    outgoing = jnp.broadcast_to(packed, (experts, 2, capacity, width)).reshape(
        devices_ep, capacity, width
    )
    received = lax.all_to_all(outgoing, "ep", split_axis=0, concat_axis=0, tiled=True)
    result = expert_half(received.reshape(-1, width), gate_weight[0], up_weight[0], down_weight[0])
    partial_value = result.reshape(received.shape[0], received.shape[1], width)
    parity = lax.axis_index("ep") % 2
    halves = partial_value.reshape(devices_ep, capacity, 2, width // 2)
    kept_half = lax.dynamic_index_in_dim(halves, parity, 2, keepdims=False)
    given_half = lax.dynamic_index_in_dim(halves, 1 - parity, 2, keepdims=False)
    partner = swapped(given_half, "ep", 0)
    reduced = (kept_half.astype(jnp.float32) + partner.astype(jnp.float32)).astype(jnp.bfloat16)
    returned = lax.all_to_all(reduced, "ep", split_axis=0, concat_axis=0, tiled=True)
    ordered = returned.reshape(experts, 2, capacity, width // 2).transpose(0, 2, 1, 3)
    expert_out = ordered.reshape(experts * capacity, width)
    picked = jnp.take(expert_out, slot_index.reshape(-1), axis=0).reshape(
        tok_count, top_count, width
    )
    weights = gate_fixed.astype(jnp.float32) / 65536.0
    mixed = jnp.sum(weights[:, :, None] * picked.astype(jnp.float32), axis=1)
    return mixed.astype(jnp.bfloat16)


def pack_tokens(tokens, routes, gate_fixed, experts):
    count, width = tokens.shape
    top = routes.shape[1]

    def kernel(tok_ref, route_ref, gate_ref, out_ref):
        rows = lax.broadcasted_iota(jnp.int32, (experts, count), 0)
        share = jnp.zeros((experts, count), jnp.float32)
        for k in range(top):
            value = gate_ref[k : k + 1, :].astype(jnp.float32) * (1.0 / 65536.0)
            share = share + jnp.where(route_ref[k : k + 1, :] == rows, value, 0.0)
        high = share.astype(jnp.bfloat16)
        low = (share - high.astype(jnp.float32)).astype(jnp.bfloat16)
        both = jnp.concatenate([high.astype(jnp.float32), low.astype(jnp.float32)], axis=0)
        unit = (
            lax.broadcasted_iota(jnp.int32, (count, count), 0)
            == lax.broadcasted_iota(jnp.int32, (count, count), 1)
        ).astype(jnp.bfloat16)
        columns = lax.dot_general(
            unit,
            both.astype(jnp.bfloat16),
            (((1,), (1,)), ((), ())),
            preferred_element_type=jnp.float32,
        )
        out_ref[:, :width] = tok_ref[...]
        out_ref[:, width:] = columns.astype(jnp.bfloat16)

    return pl.pallas_call(
        kernel,
        out_shape=jax.ShapeDtypeStruct((count, width + 2 * experts), jnp.bfloat16),
        in_specs=[pl.BlockSpec(memory_space=pltpu.VMEM)] * 3,
        out_specs=pl.BlockSpec(memory_space=pltpu.VMEM),
        compiler_params=pltpu.CompilerParams(vmem_limit_bytes=2 * 2**20),
        name="pack_tokens",
    )(tokens, routes.T, gate_fixed.T)


def fetched(weights):
    pieces = 3

    def kernel(*refs):
        number = len(weights)
        copies = []
        for n in range(number):
            rows = weights[n].shape[0] // pieces // 16 * 16
            for m in range(pieces):
                start = m * rows
                size = rows if m < pieces - 1 else weights[n].shape[0] - start
                copies.append(
                    pltpu.make_async_copy(
                        refs[n].at[pl.ds(start, size)],
                        refs[number + n].at[pl.ds(start, size)],
                        refs[2 * number].at[n * pieces + m],
                    )
                )
        for copy in copies:
            copy.start()
        for copy in copies:
            copy.wait()

    placed = [pltpu.with_memory_space_constraint(weight, pltpu.HBM) for weight in weights]
    return pl.pallas_call(
        kernel,
        out_shape=[pltpu.VMEM(weight.shape, weight.dtype) for weight in weights],
        in_specs=[pl.BlockSpec(memory_space=pl.ANY)] * len(weights),
        out_specs=[pl.BlockSpec(memory_space=pltpu.VMEM)] * len(weights),
        scratch_shapes=[pltpu.SemaphoreType.DMA((pieces * len(weights),))],
        compiler_params=pltpu.CompilerParams(vmem_limit_bytes=2**20),
        name="fetch",
    )(*placed)


def expert_chunks(chunks, expert, w_gate, w_up, w_down, width):
    count = chunks[0].shape[0]
    wide = chunks[0].shape[1]
    experts = (wide - width) // 2
    number = len(chunks)
    rows = number * count
    tail = width // 128 * 128
    step = 768

    def kernel(*refs):
        expert_ref = refs[0]
        in_refs = refs[1 : 1 + number]
        wg_ref, wu_ref, wd_ref = refs[1 + number : 4 + number]
        out_refs = refs[4 + number : 4 + 2 * number]
        x_ref = refs[4 + 2 * number]
        for n in range(number):
            x_ref[n * count : (n + 1) * count, :] = in_refs[n][...]
        lanes = lax.broadcasted_iota(jnp.int32, (8, wide - tail), 1) - (width - tail)
        mine = (lanes == expert_ref[0]) | (lanes == expert_ref[0] + experts)
        nt = (((1,), (1,)), ((), ()))
        share = lax.dot_general(
            jnp.where(mine, 1.0, 0.0).astype(jnp.bfloat16),
            x_ref[:, tail:],
            nt,
            preferred_element_type=jnp.float32,
        )[0:1, :]
        x = x_ref[:, :width]
        gate = lax.dot_general(wg_ref[...], x, nt, preferred_element_type=jnp.float32)
        up = lax.dot_general(wu_ref[...], x, nt, preferred_element_type=jnp.float32)
        hidden = gate / (1.0 + jnp.exp(-gate)) * up * share
        hidden = hidden.T.astype(jnp.bfloat16)
        for start in range(0, width, step):
            size = min(step, width - start)
            part = jnp.dot(
                hidden, wd_ref[:, start : start + size], preferred_element_type=jnp.float32
            ).astype(jnp.bfloat16)
            for m in range(number):
                out_refs[m][:, start : start + size] = part[m * count : (m + 1) * count, :]

    vmem = pl.BlockSpec(memory_space=pltpu.VMEM)
    return pl.pallas_call(
        kernel,
        out_shape=[jax.ShapeDtypeStruct((count, width), jnp.bfloat16)] * number,
        in_specs=[pl.BlockSpec(memory_space=pltpu.SMEM)] + [vmem] * (number + 3),
        out_specs=[vmem] * number,
        scratch_shapes=[pltpu.VMEM((rows, wide), jnp.bfloat16)],
        compiler_params=pltpu.CompilerParams(vmem_limit_bytes=16 * 2**20),
        name="expert_chunks",
    )(expert, *chunks, w_gate, w_up, w_down)


def added(*values):
    total = values[0].astype(jnp.float32)
    for value in values[1:]:
        total = total + value.astype(jnp.float32)
    return total.astype(jnp.bfloat16)


def dense(tokens, routes, gate_fixed, gate_weight, up_weight, down_weight):
    devices_ep = lax.axis_size("ep")
    layers = devices_ep // 4
    width = tokens.shape[1]
    expert = jnp.right_shift(lax.axis_index("ep").astype(jnp.int32), 1).reshape(1)
    tokens, expert = lax.optimization_barrier((tokens, expert))
    own = pack_tokens(tokens, routes, gate_fixed, devices_ep // 2)
    near = [own] + [turned(own, "ep", k) for k in range(1, layers)]
    far = [swapped(near[k], "ep", 1) for k in range(layers)]
    mine = near + far
    theirs = [swapped(mine[k], "ep", 0) for k in range(len(mine))]
    w_gate, w_up, w_down = fetched([gate_weight[0].T, up_weight[0].T, down_weight[0]])
    parts = expert_chunks(mine + theirs, expert, w_gate, w_up, w_down, width)
    kept, given = parts[: len(mine)], parts[len(mine) :]
    back = [swapped(given[k], "ep", 0) for k in range(len(given))]
    far_sums = [added(kept[layers + k], back[layers + k]) for k in range(layers)]
    from_far = [swapped(far_sums[k], "ep", 1) for k in range(layers)]
    near_sums = [added(kept[k], back[k], from_far[k]) for k in range(layers)]
    home = [turned(near_sums[k], "ep", -k) for k in range(1, layers)]
    return added(kept[0], back[0], from_far[0], *home)


def local(tokens, routes, gate_fixed, gate_weight, up_weight, down_weight):
    devices_ep = lax.axis_size("ep")
    tok_count, top_count = routes.shape
    capacity = min(tok_count, 2 * tok_count * top_count // (devices_ep // 2))
    if capacity == tok_count and devices_ep % 4 == 0:
        return dense(tokens, routes, gate_fixed, gate_weight, up_weight, down_weight)
    return slotted(tokens, routes, gate_fixed, gate_weight, up_weight, down_weight, capacity)


def solution(mesh):
    placed = (
        P(("groups", "ep"), None),
        P(("groups", "ep"), None),
        P(("groups", "ep"), None),
        P("ep", None, None),
        P("ep", None, None),
        P("ep", None, None),
    )
    return jax.shard_map(
        local, mesh=mesh, in_specs=placed, out_specs=P(("groups", "ep"), None), check_vma=False
    )
```

```python
import jax
import jax.numpy as jnp
from jax import lax
from jax.experimental import pallas as pl
from jax.experimental.pallas import tpu as pltpu
from jax.sharding import PartitionSpec as P


def swapped(value, axis, bit):
    mask = 2**bit
    pairs = [(source, source ^ mask) for source in range(lax.axis_size(axis))]
    return lax.ppermute(value, axis, pairs)


def moved(value, axis, mask):
    pairs = [(source, source ^ mask) for source in range(lax.axis_size(axis))]
    return lax.ppermute(value, axis, pairs)


def expert_half(expert_rows, w_gate, w_up, w_down):
    gate_part = jnp.dot(expert_rows, w_gate, preferred_element_type=jnp.float32)
    up_part = jnp.dot(expert_rows, w_up, preferred_element_type=jnp.float32)
    hidden = (jax.nn.silu(gate_part) * up_part).astype(jnp.bfloat16)
    return jnp.dot(hidden, w_down, preferred_element_type=jnp.float32).astype(jnp.bfloat16)


def slotted(tokens, routes, gate_fixed, gate_weight, up_weight, down_weight, capacity):
    devices_ep = lax.axis_size("ep")
    experts = devices_ep // 2
    tok_count = tokens.shape[0]
    top_count = routes.shape[1]
    width = tokens.shape[1]
    onehot = (routes[:, :, None] == jnp.arange(experts, dtype=jnp.int32)).astype(jnp.int32)
    flat_hot = onehot.reshape(tok_count * top_count, experts)
    before = jnp.cumsum(flat_hot, axis=0) - flat_hot
    position = jnp.sum(before * flat_hot, axis=1).reshape(tok_count, top_count)
    slot_index = routes * capacity + position
    select = (slot_index[:, :, None] == jnp.arange(experts * capacity, dtype=jnp.int32)).astype(
        jnp.int32
    )
    select = jnp.sum(select, axis=1).astype(jnp.bfloat16)
    packed = jnp.einsum("ts,td->sd", select, tokens, preferred_element_type=jnp.float32).astype(
        jnp.bfloat16
    )
    packed = packed.reshape(experts, 1, capacity, width)
    outgoing = jnp.broadcast_to(packed, (experts, 2, capacity, width)).reshape(
        devices_ep, capacity, width
    )
    received = lax.all_to_all(outgoing, "ep", split_axis=0, concat_axis=0, tiled=True)
    result = expert_half(received.reshape(-1, width), gate_weight[0], up_weight[0], down_weight[0])
    partial_value = result.reshape(received.shape[0], received.shape[1], width)
    parity = lax.axis_index("ep") % 2
    halves = partial_value.reshape(devices_ep, capacity, 2, width // 2)
    kept_half = lax.dynamic_index_in_dim(halves, parity, 2, keepdims=False)
    given_half = lax.dynamic_index_in_dim(halves, 1 - parity, 2, keepdims=False)
    partner = swapped(given_half, "ep", 0)
    reduced = (kept_half.astype(jnp.float32) + partner.astype(jnp.float32)).astype(jnp.bfloat16)
    returned = lax.all_to_all(reduced, "ep", split_axis=0, concat_axis=0, tiled=True)
    ordered = returned.reshape(experts, 2, capacity, width // 2).transpose(0, 2, 1, 3)
    expert_out = ordered.reshape(experts * capacity, width)
    picked = jnp.take(expert_out, slot_index.reshape(-1), axis=0).reshape(
        tok_count, top_count, width
    )
    weights = gate_fixed.astype(jnp.float32) / 65536.0
    mixed = jnp.sum(weights[:, :, None] * picked.astype(jnp.float32), axis=1)
    return mixed.astype(jnp.bfloat16)


def pack_tokens(tokens, routes, gate_fixed, experts):
    count, width = tokens.shape
    top = routes.shape[1]

    def kernel(tok_hbm, route_hbm, gate_hbm, out_ref, tok_ref, route_ref, gate_ref, sem):
        copies = [
            pltpu.make_async_copy(source, place, sem.at[n])
            for n, (source, place) in enumerate(
                ((tok_hbm, tok_ref), (route_hbm, route_ref), (gate_hbm, gate_ref))
            )
        ]
        for copy in copies:
            copy.start()
        copies[1].wait()
        copies[2].wait()
        rows = lax.broadcasted_iota(jnp.int32, (experts, count), 0)
        share = jnp.zeros((experts, count), jnp.float32)
        for k in range(top):
            value = gate_ref[k : k + 1, :].astype(jnp.float32) * (1.0 / 65536.0)
            share = share + jnp.where(route_ref[k : k + 1, :] == rows, value, 0.0)
        high = share.astype(jnp.bfloat16)
        low = (share - high.astype(jnp.float32)).astype(jnp.bfloat16)
        both = jnp.concatenate([high.astype(jnp.float32), low.astype(jnp.float32)], axis=0)
        unit = (
            lax.broadcasted_iota(jnp.int32, (count, count), 0)
            == lax.broadcasted_iota(jnp.int32, (count, count), 1)
        ).astype(jnp.bfloat16)
        columns = lax.dot_general(
            unit,
            both.astype(jnp.bfloat16),
            (((1,), (1,)), ((), ())),
            preferred_element_type=jnp.float32,
        )
        copies[0].wait()
        out_ref[:, :width] = tok_ref[...]
        out_ref[:, width:] = columns.astype(jnp.bfloat16)

    given = [
        pltpu.with_memory_space_constraint(value, pltpu.HBM)
        for value in (tokens, routes.T, gate_fixed.T)
    ]
    return pl.pallas_call(
        kernel,
        out_shape=pltpu.VMEM((count, width + 2 * experts), jnp.bfloat16),
        in_specs=[pl.BlockSpec(memory_space=pl.ANY)] * 3,
        out_specs=pl.BlockSpec(memory_space=pltpu.VMEM),
        scratch_shapes=[pltpu.VMEM(value.shape, value.dtype) for value in given]
        + [pltpu.SemaphoreType.DMA((3,))],
        compiler_params=pltpu.CompilerParams(vmem_limit_bytes=2 * 2**20),
        name="pack_tokens",
    )(*given)


def fetched(weights):
    pieces = 6

    def kernel(*refs):
        number = len(weights)
        copies = []
        for n in range(number):
            rows = weights[n].shape[0] // pieces // 16 * 16
            for m in range(pieces):
                start = m * rows
                size = rows if m < pieces - 1 else weights[n].shape[0] - start
                copies.append(
                    pltpu.make_async_copy(
                        refs[n].at[pl.ds(start, size)],
                        refs[number + n].at[pl.ds(start, size)],
                        refs[2 * number].at[n * pieces + m],
                    )
                )
        for copy in copies:
            copy.start()
        for copy in copies:
            copy.wait()

    placed = [pltpu.with_memory_space_constraint(weight, pltpu.HBM) for weight in weights]
    return pl.pallas_call(
        kernel,
        out_shape=[pltpu.VMEM(weight.shape, weight.dtype) for weight in weights],
        in_specs=[pl.BlockSpec(memory_space=pl.ANY)] * len(weights),
        out_specs=[pl.BlockSpec(memory_space=pltpu.VMEM)] * len(weights),
        scratch_shapes=[pltpu.SemaphoreType.DMA((pieces * len(weights),))],
        compiler_params=pltpu.CompilerParams(vmem_limit_bytes=2**20),
        name="fetch",
    )(*placed)


def expert_chunks(chunks, expert, weights, inside, width):
    count = chunks[0].shape[0]
    wide = chunks[0].shape[1]
    experts = (wide - width) // 2
    number = len(chunks)
    rows = number * count
    half, quarter = rows // 2, rows // 4
    units = weights[0].shape[0]
    tail = width // 128 * 128
    step = 768
    pieces = 3
    piece = units // pieces // 16 * 16
    outside = [n for n in range(3) if not inside[n]]

    def kernel(*refs):
        expert_ref = refs[0]
        in_refs = refs[1 : 1 + number]
        w_refs = list(refs[1 + number : 4 + number])
        kept_ref, far_ref, near_ref, x_ref, g_ref, h_ref = refs[4 + number : 10 + number]
        spare, sem = refs[10 + number : -1], refs[-1]
        copies = {}
        for m, n in enumerate(outside):
            copies[n] = []
            for k in range(pieces):
                span = pl.ds(k * piece, piece if k < pieces - 1 else units - k * piece)
                copies[n].append(
                    pltpu.make_async_copy(
                        w_refs[n].at[span], spare[m].at[span], sem.at[m * pieces + k]
                    )
                )
                copies[n][-1].start()
            w_refs[n] = spare[m]
        for n in range(number):
            x_ref[n * count : (n + 1) * count, :] = in_refs[n][...]
        nt = (((1,), (1,)), ((), ()))

        def ready(n):
            for copy in copies.get(n, ()):
                copy.wait()

        @pl.when(expert_ref[0] >= 0)
        def _():
            ready(0)
            g_ref[...] = lax.dot_general(
                w_refs[0][...], x_ref[:, :width], nt, preferred_element_type=jnp.float32
            )

        @pl.when(expert_ref[0] >= 0)
        def _():
            ready(1)
            lanes = lax.broadcasted_iota(jnp.int32, (8, wide - tail), 1) - (width - tail)
            mine = (lanes == expert_ref[0]) | (lanes == expert_ref[0] + experts)
            share = lax.dot_general(
                jnp.where(mine, 1.0, 0.0).astype(jnp.bfloat16),
                x_ref[:, tail:],
                nt,
                preferred_element_type=jnp.float32,
            )[0:1, :]
            up = lax.dot_general(
                w_refs[1][...], x_ref[:, :width], nt, preferred_element_type=jnp.float32
            )
            gate = g_ref[...]
            hidden = gate / (1.0 + jnp.exp(-gate)) * up * share
            h_ref[...] = hidden.T.astype(jnp.bfloat16)

        @pl.when(expert_ref[0] >= 0)
        def _():
            ready(2)
            hidden = h_ref[...]
            for start in range(0, width, step):
                stop = min(start + step, width)
                part = jnp.dot(
                    hidden, w_refs[2][:, start:stop], preferred_element_type=jnp.float32
                )
                kept_ref[:, start:stop] = part[:half, :]
                far_ref[:, start:stop] = part[half : half + quarter, :].astype(jnp.bfloat16)
                near_ref[:, start:stop] = part[half + quarter :, :].astype(jnp.bfloat16)

    vmem = pl.BlockSpec(memory_space=pltpu.VMEM)
    placed = [
        weights[n] if inside[n] else pltpu.with_memory_space_constraint(weights[n], pltpu.HBM)
        for n in range(3)
    ]
    return pl.pallas_call(
        kernel,
        out_shape=[
            pltpu.VMEM((half, width), jnp.float32),
            pltpu.VMEM((quarter, width), jnp.bfloat16),
            pltpu.VMEM((quarter, width), jnp.bfloat16),
        ],
        in_specs=[pl.BlockSpec(memory_space=pltpu.SMEM)]
        + [vmem] * number
        + [vmem if inside[n] else pl.BlockSpec(memory_space=pl.ANY) for n in range(3)],
        out_specs=[vmem] * 3,
        scratch_shapes=[
            pltpu.VMEM((rows, wide), jnp.bfloat16),
            pltpu.VMEM((units, rows), jnp.float32),
            pltpu.VMEM((rows, units), jnp.bfloat16),
        ]
        + [pltpu.VMEM(weights[n].shape, weights[n].dtype) for n in outside]
        + [pltpu.SemaphoreType.DMA((max(1, pieces * len(outside)),))],
        compiler_params=pltpu.CompilerParams(vmem_limit_bytes=32 * 2**20),
        name="expert_chunks",
    )(expert, *chunks, *placed)


def added(*values):
    total = values[0].astype(jnp.float32)
    for value in values[1:]:
        total = total + value.astype(jnp.float32)
    return total.astype(jnp.bfloat16)


def apart(*values):
    return lax.optimization_barrier(values)


def dense(tokens, routes, gate_fixed, gate_weight, up_weight, down_weight):
    devices_ep = lax.axis_size("ep")
    layers = devices_ep // 4
    width = tokens.shape[1]
    expert = jnp.right_shift(lax.axis_index("ep").astype(jnp.int32), 1).reshape(1)
    tokens, expert = lax.optimization_barrier((tokens, expert))
    own = pack_tokens(tokens, routes, gate_fixed, devices_ep // 2)
    straight, groups = (1,), ((2,), (3,), (0,))
    order = [k for group in groups for k in group] + list(straight)
    near = [own] + [moved(own, "ep", 4 * k) for k in range(1, layers)]
    far = [
        moved(own, "ep", 4 * k + 2)
        if k in straight
        else moved(near[k], "ep", 2)
        for k in range(layers)
    ]
    mine = [far[k] for k in order] + [near[k] for k in order]
    theirs = [moved(mine[k], "ep", 1) for k in range(len(mine))]
    weights = [gate_weight[0].T, up_weight[0].T, down_weight[0]]
    inside = [False] * 3
    found = fetched([weights[k] for k in (0,)])
    for k, value in zip((0,), found):
        weights[k], inside[k] = value, True
    found = fetched([weights[k] for k in (1,)])
    for k, value in zip((1,), found):
        weights[k], inside[k] = value, True
    kept, far_given, near_given = expert_chunks(
        mine + theirs, expert, weights, inside, width
    )
    far_back = moved(far_given, "ep", 1)
    near_back = moved(near_given, "ep", 1)
    count = tokens.shape[0]
    kept_near = kept[layers * count :]

    def rows(start, stop):
        return slice(start * count, stop * count)

    from_far = {}
    first = 0
    for group in groups:
        cut = rows(first, first + len(group))
        value = added(*apart(kept[cut], far_back[cut]))
        value = moved(value, "ep", 2)
        for m, k in enumerate(group):
            from_far[k] = value[rows(m, m + 1)]
        first += len(group)
    home = []
    for n, k in enumerate(order):
        cut = rows(n, n + 1)
        if k in straight:
            value = added(*apart(kept[cut], far_back[cut]))
            home.append(moved(value, "ep", 4 * k + 2))
            parts = apart(kept_near[cut], near_back[cut])
        else:
            parts = apart(kept_near[cut], near_back[cut], from_far[k])
        if k:
            value = added(*parts)
            home.append(moved(value, "ep", 4 * k))
        else:
            home.extend(parts)
    return added(*home)


def local(tokens, routes, gate_fixed, gate_weight, up_weight, down_weight):
    devices_ep = lax.axis_size("ep")
    tok_count, top_count = routes.shape
    capacity = min(tok_count, 2 * tok_count * top_count // (devices_ep // 2))
    if capacity == tok_count and devices_ep in (4, 8, 16, 32, 64):
        return dense(tokens, routes, gate_fixed, gate_weight, up_weight, down_weight)
    return slotted(tokens, routes, gate_fixed, gate_weight, up_weight, down_weight, capacity)


def solution(mesh):
    placed = (
        P(("groups", "ep"), None),
        P(("groups", "ep"), None),
        P(("groups", "ep"), None),
        P("ep", None, None),
        P("ep", None, None),
        P("ep", None, None),
    )
    return jax.shard_map(
        local, mesh=mesh, in_specs=placed, out_specs=P(("groups", "ep"), None), check_vma=False
    )
```
